256 devices in a mesh: seq: 32 (over y, z), head: 8 (over x, core).
Axes of the slice: x: 4, y: 4, z: 8, core: 2. Of those that a mesh axis runs over, the one named last changes fastest.
Arguments:
- query_rows: bfloat16 [32768, 4096], P('seq', 'head'), may hold values from -6 to 6
- key_rows: bfloat16 [32768, 4096], P('seq', 'head'), may hold values from -6 to 6
- value_rows: bfloat16 [32768, 4096], P('seq', 'head'), may hold values from -15 to 15
- block_picks: int32 [64, 32, 4], P('seq', 'head'), may hold values from -1 to 63, as said below
- out_weight: bfloat16 [4096, 4096], P(None, 'head'), may hold values from -0.09375 to 0.09375
Outputs:
- mixed: bfloat16 [32768, 4096], P('seq', 'head')
The draws below stay inside these ranges and needn't reach their ends.
Inputs may be any that keep to these rules, and one draw needn't show every extreme that they name: `block_picks`: every entry that is not -1 names a block held by a lower index of seq than block b. Repeated entries of one row count once. Over the query blocks of one index of seq and the heads of one index of head, at most 2 entries name blocks of any one other index of seq, and every index of seq from 1 on has exactly 2 entries naming blocks of index 0.
All inputs are finite; a program needn't handle non-finite values.
Results may differ from the reference program's by a relative error of at most 0.0059.
Values may be sent and summed in bfloat16 or wider, within the bound.
No kernel may reach another device: no remote copies, remote signals or barrier semaphores. Data moves between devices by JAX's collectives and lax.ppermute only.
A program may use at most 192 MiB of HBM per device.

```python
import jax
import jax.numpy as jnp
import numpy as np
from jax import lax

HEADS = 32
HEAD_DIM = 128
D = 4096
BLOCK = 512
TOPK = 5
CAP = 2
BLK_DEV = 2
SEQ = 32768
N_SEQ = 32
N_HEAD = 8


def drawn_pair(key):
    row_count = BLK_DEV * BLOCK * N_SEQ
    width_all = HEADS * HEAD_DIM
    streams = jax.random.split(jax.random.fold_in(key, 7001), 2)
    queries = jnp.clip(1.5 * jax.random.normal(streams[0], (row_count, width_all), jnp.float32), -6.0, 6.0)
    keys_drawn = jnp.clip(1.5 * jax.random.normal(streams[1], (row_count, width_all), jnp.float32), -6.0, 6.0)
    return (queries, keys_drawn)


def draw_query_rows(key, part):
    return drawn_pair(key)[0].astype(jnp.bfloat16)


def draw_key_rows(key, part):
    return drawn_pair(key)[1].astype(jnp.bfloat16)


def draw_block_picks(key, part):
    group_heads = HEADS // N_HEAD
    pair_count = BLK_DEV * group_heads
    slot_count = TOPK - 1
    entry_count = pair_count * slot_count
    seat_count = (N_SEQ - 1) * CAP
    later_count = entry_count - CAP
    later_entries = jnp.asarray(np.array([index_value for index_value in range(entry_count) if index_value % slot_count != 0], dtype=np.int32))

    def one_list(group_id, requester):
        list_key = jax.random.fold_in(jax.random.fold_in(key, 9103), group_id * N_SEQ + requester)
        streams = jax.random.split(list_key, 4)
        first_entries = jax.random.permutation(streams[0], pair_count).astype(jnp.int32) * slot_count
        later_order = jax.random.permutation(streams[1], later_entries).astype(jnp.int32)
        order_list = jnp.concatenate([first_entries, later_order])
        seat_perm = jax.random.permutation(streams[2], seat_count).astype(jnp.int32)
        seat_owner = seat_perm // CAP + 1
        blocked = (seat_owner >= requester).astype(jnp.int32)
        ranked = jnp.argsort(blocked * seat_count + jnp.arange(seat_count, dtype=jnp.int32))
        usable_count = jnp.sum(1 - blocked)
        sorted_owner = jnp.concatenate([seat_owner[ranked], jnp.full((later_count,), -1, jnp.int32)])
        position = jnp.arange(later_count, dtype=jnp.int32)
        later_owner = jnp.where(position < usable_count, sorted_owner[position], -1)
        hot_owner = jnp.where(requester >= 1, jnp.zeros((CAP,), jnp.int32), -1)
        owners = jnp.concatenate([hot_owner, later_owner])
        within = jax.random.randint(streams[3], (entry_count,), 0, BLK_DEV).astype(jnp.int32)
        chosen = jnp.where(owners >= 0, owners * BLK_DEV + within, -1)
        listed = jnp.zeros((entry_count,), jnp.int32).at[order_list].set(chosen)
        return listed.reshape(BLK_DEV, group_heads, slot_count)
    requesters = jnp.arange(N_SEQ, dtype=jnp.int32)
    all_lists = jax.vmap(lambda group_id: jax.vmap(lambda requester: one_list(group_id, requester))(requesters))(jnp.arange(N_HEAD, dtype=jnp.int32))
    all_lists = jnp.transpose(all_lists, (1, 2, 0, 3, 4))
    return all_lists.reshape(N_SEQ * BLK_DEV, HEADS, slot_count)


def block_scale(stream_key, extent, pieces, smallest, high):
    def one(axis_at, shards_of):
        draws = jax.random.uniform(jax.random.fold_in(jax.random.fold_in(stream_key, 6), axis_at), (shards_of,), jnp.float32, smallest / len(pieces), high / len(pieces))
        return jnp.repeat(jnp.exp(draws), extent[axis_at] // shards_of).reshape((-1,) + (1,) * (len(extent) - axis_at - 1))

    factor_of = one(*pieces[0])
    for cut in pieces[1:]:
        factor_of = factor_of * one(*cut)
    return factor_of


def gaussian(rng, dims, deviation, bound, shards=(), held_as=jnp.bfloat16):
    drawn = deviation * jax.random.normal(rng, dims, jnp.float32)
    if shards:
        drawn = drawn * block_scale(rng, dims, shards, -0.22, 0.18)
    return jnp.clip(drawn, -bound, bound).astype(held_as)


def setup_inputs(seed: int = 0) -> dict:
    key_of = jax.random.split(jax.random.key(seed), 6)
    query_rows = draw_query_rows(jax.random.fold_in(key_of[5], 71), 0)
    key_rows = draw_key_rows(jax.random.fold_in(key_of[5], 71), 0)
    value_rows = gaussian(key_of[2], (SEQ, HEADS * HEAD_DIM), 3.0, 15.0, ((0, 32), (1, 8)))
    block_picks = draw_block_picks(jax.random.fold_in(key_of[5], 71), 0)
    out_weight = gaussian(key_of[4], (HEADS * HEAD_DIM, D), (HEADS * HEAD_DIM) ** -0.5, 0.09375, ((1, 8),))
    return {"query_rows": query_rows, "key_rows": key_rows, "value_rows": value_rows, "block_picks": block_picks, "out_weight": out_weight}


def block_partial(query_tile, key_tile, value_tile, causal_mask):
    score_scale = HEAD_DIM ** -0.5
    scores = jnp.einsum("hqd,hkd->hqk", query_tile.astype(jnp.float32), key_tile.astype(jnp.float32)) * score_scale
    if causal_mask is not None:
        scores = jnp.where(causal_mask, scores, -jnp.inf)
    maxima = jnp.max(scores, axis=-1)
    shifted = jnp.exp(scores - maxima[..., None])
    totals = jnp.sum(shifted, axis=-1)
    weights = shifted.astype(jnp.bfloat16)
    partial_out = jnp.einsum("hqk,hkd->hqd", weights.astype(jnp.float32), value_tile.astype(jnp.float32))
    return partial_out.astype(jnp.bfloat16), maxima, totals


def merge_parts(outputs, maxima, totals, usable):
    keep = usable[:, :, None]
    largest = jnp.max(jnp.where(keep, maxima, -jnp.inf), axis=0)
    factor = jnp.where(keep, jnp.exp(maxima - largest[None]), 0.0)
    numer = jnp.sum(factor[..., None] * outputs.astype(jnp.float32), axis=0)
    denom = jnp.sum(factor * totals, axis=0)
    return (numer / denom[..., None]).astype(jnp.bfloat16)


def reference(query_rows, key_rows, value_rows, block_picks, out_weight):
    block_count = query_rows.shape[0] // BLOCK
    block_shape = (block_count, BLOCK, HEADS, HEAD_DIM)
    queries = query_rows.reshape(block_shape)
    key_blocks = key_rows.reshape(block_shape)
    value_blocks = value_rows.reshape(block_shape)
    positions = jnp.arange(BLOCK)
    causal_mask = positions[:, None] >= positions[None, :]
    head_index = jnp.arange(HEADS)

    def one_block(block_id):
        query_tile = jnp.transpose(queries[block_id], (1, 0, 2))
        own_part = block_partial(query_tile, jnp.transpose(key_blocks[block_id], (1, 0, 2)),
                                 jnp.transpose(value_blocks[block_id], (1, 0, 2)), causal_mask)
        chosen = block_picks[block_id]
        part_outputs = [own_part[0]]
        part_maxima = [own_part[1]]
        part_totals = [own_part[2]]
        part_usable = [jnp.ones((HEADS,), dtype=jnp.bool_)]
        for column in range(chosen.shape[1]):
            entries = chosen[:, column]
            usable = entries >= 0
            for earlier in range(column):
                usable = usable & (entries != chosen[:, earlier])
            safe_index = jnp.where(usable, entries, 0)
            result_part = block_partial(query_tile, key_blocks[safe_index, :, head_index, :],
                                        value_blocks[safe_index, :, head_index, :], None)
            part_outputs.append(result_part[0])
            part_maxima.append(result_part[1])
            part_totals.append(result_part[2])
            part_usable.append(usable)
        combined = merge_parts(jnp.stack(part_outputs), jnp.stack(part_maxima), jnp.stack(part_totals),
                               jnp.stack(part_usable))
        return jnp.transpose(combined, (1, 0, 2)).reshape(BLOCK, HEADS * HEAD_DIM)

    attended = lax.map(one_block, jnp.arange(block_count, dtype=jnp.int32)).reshape(-1, HEADS * HEAD_DIM)
    return jnp.dot(attended, out_weight, preferred_element_type=jnp.float32).astype(jnp.bfloat16)
```

```python
import functools

import jax
import jax.numpy as jnp
from jax import lax
from jax.experimental import pallas as pl
from jax.experimental.pallas import tpu as pltpu
from jax.sharding import Mesh
from jax.sharding import PartitionSpec as P

LOG2E = 1.4426950408889634
CHUNK = 256


def attend_kernel(kidx_ref, valid_ref, q_ref, k_ref, v_ref, o_ref, m_ref, l_ref, acc_ref, *, slots, scale):
    qb = pl.program_id(0)
    slot = pl.program_id(1)
    rows = q_ref.shape[1]

    def step(first):
        keys = k_ref[0, 0]
        values = v_ref[0, 0]
        for c in range(rows // CHUNK):
            cols = slice(c * CHUNK, (c + 1) * CHUNK)
            scores = lax.dot_general(
                keys, q_ref[0, cols, :], (((1,), (1,)), ((), ())), preferred_element_type=jnp.float32
            )
            if first:
                kpos = lax.broadcasted_iota(jnp.int32, scores.shape, 0)
                qpos = lax.broadcasted_iota(jnp.int32, scores.shape, 1) + c * CHUNK
                scores = jnp.where(kpos <= qpos, scores, -jnp.inf)
            top = jnp.max(scores, axis=0, keepdims=True)
            if not first:
                old = m_ref[:, cols]
                top = jnp.maximum(top, old)
            weights = jnp.exp2((scores - top) * (scale * LOG2E))
            total = jnp.sum(weights, axis=0, keepdims=True)
            part = lax.dot_general(
                values, weights.astype(jnp.bfloat16), (((0,), (0,)), ((), ())),
                preferred_element_type=jnp.float32,
            )
            m_ref[:, cols] = top
            if first:
                l_ref[:, cols] = total
                acc_ref[:, cols] = part
            else:
                factor = jnp.exp2((old - top) * (scale * LOG2E))
                l_ref[:, cols] = l_ref[:, cols] * factor + total
                acc_ref[:, cols] = acc_ref[:, cols] * factor + part

    @pl.when(slot == 0)
    def _():
        step(True)

    @pl.when((slot > 0) & (valid_ref[qb * slots + slot] > 0))
    def _():
        step(False)

    @pl.when(slot == slots - 1)
    def _():
        o_ref[0] = (acc_ref[...] / l_ref[...]).T.astype(o_ref.dtype)


def attend(kidx, valid, queries, kv, slots):
    n, rows, width = queries.shape
    grid_spec = pltpu.PrefetchScalarGridSpec(
        num_scalar_prefetch=2,
        grid=(n, slots),
        in_specs=[
            pl.BlockSpec((1, rows, width), lambda q, s, kidx, valid: (q, 0, 0)),
            pl.BlockSpec((1, 1, rows, width), lambda q, s, kidx, valid: (kidx[q * slots + s], 0, 0, 0)),
            pl.BlockSpec((1, 1, rows, width), lambda q, s, kidx, valid: (kidx[q * slots + s], 1, 0, 0)),
        ],
        out_specs=pl.BlockSpec((1, rows, width), lambda q, s, kidx, valid: (q, 0, 0)),
        scratch_shapes=[
            pltpu.VMEM((1, rows), jnp.float32),
            pltpu.VMEM((1, rows), jnp.float32),
            pltpu.VMEM((width, rows), jnp.float32),
        ],
    )
    flops = n * slots * 4 * rows * rows * width
    return pl.pallas_call(
        functools.partial(attend_kernel, slots=slots, scale=width**-0.5),
        out_shape=jax.ShapeDtypeStruct((n, rows, width), jnp.bfloat16),
        grid_spec=grid_spec,
        cost_estimate=pl.CostEstimate(
            flops=flops, bytes_accessed=n * slots * 4 * rows * width, transcendentals=n * slots * rows * rows
        ),
        compiler_params=pltpu.CompilerParams(dimension_semantics=("arbitrary", "arbitrary")),
    )(kidx, valid, queries, kv, kv)


def body(query_rows, key_rows, value_rows, block_picks, out_weight):
    ny, nz, nc = lax.axis_size("y"), lax.axis_size("z"), lax.axis_size("c")
    y, z, c = lax.axis_index("y"), lax.axis_index("z"), lax.axis_index("c")
    tok_rows, feature = query_rows.shape
    blocks, heads, picks = block_picks.shape
    rows, width = tok_rows // blocks, feature // heads

    def tiles(rows_in):
        shaped = rows_in.reshape(blocks, rows, heads, width)
        return jnp.transpose(shaped, (0, 2, 1, 3))

    payload = jnp.stack((tiles(key_rows), tiles(value_rows), tiles(query_rows)), 2)
    payload = lax.all_to_all(payload, "c", split_axis=0, concat_axis=0, tiled=True)
    payload = payload.reshape(nz, 3, rows, width)
    payload = lax.all_to_all(payload, "z", split_axis=0, concat_axis=0, tiled=True)
    queries = payload[:, 2]
    kv = lax.all_gather(payload[:, :2], "y")
    kv = lax.all_gather(kv, "c")
    kv = kv.reshape(nc * ny * nz, 2, rows, width)

    everyone = lax.all_gather(lax.all_gather(block_picks, "c"), "z")
    mine = lax.dynamic_index_in_dim(everyone, z // heads, 1, keepdims=False)
    mine = lax.dynamic_index_in_dim(mine, c, 1, keepdims=False)
    mine = lax.dynamic_index_in_dim(mine, z % heads, 1, keepdims=False)
    valid, where = [jnp.ones((nz,), jnp.int32)], [(c * ny + y) * nz + jnp.arange(nz, dtype=jnp.int32)]
    for s in range(picks):
        entry = mine[:, s]
        fresh = entry >= 0
        for t in range(s):
            fresh = fresh & (entry != mine[:, t])
        index = ((entry % blocks) * ny + entry // (nz * blocks)) * nz + (entry // blocks) % nz
        valid.append(fresh.astype(jnp.int32))
        where.append(jnp.where(fresh, index, where[-1]))
    valid = jnp.stack(valid, 1).reshape(-1)
    where = jnp.stack(where, 1).reshape(-1)
    out = attend(where, valid, queries, kv, picks + 1)

    out = lax.all_to_all(out, "z", split_axis=0, concat_axis=0, tiled=True)
    out = jnp.transpose(out, (1, 0, 2)).reshape(rows, nz * width)
    out = lax.all_gather(out, "x", axis=1, tiled=True)
    out = lax.all_gather(out, "c", axis=0, tiled=True)
    mixed = jnp.dot(out, out_weight, preferred_element_type=jnp.float32)
    return mixed.astype(jnp.bfloat16)


def solution(mesh):
    finer = Mesh(mesh.devices.reshape(4, 8, 4, 2), ("y", "z", "x", "c"))
    seq, head = ("y", "z"), ("x", "c")
    return jax.shard_map(
        body,
        mesh=finer,
        in_specs=(
            P(seq, head),
            P(seq, head),
            P(seq, head),
            P(seq, head, None),
            P(None, head),
        ),
        out_specs=P(seq, head),
        check_vma=False,
    )
```

```python
import functools

import jax
import jax.numpy as jnp
from jax import lax
from jax.experimental import pallas as pl
from jax.experimental.pallas import tpu as pltpu
from jax.sharding import Mesh
from jax.sharding import PartitionSpec as P

LOG2E = 1.4426950408889634
CHUNK = 256
PAD = 16


def shift(array, axis, by):
    size = lax.axis_size(axis)
    return lax.ppermute(array, axis, [(i, (i + by) % size) for i in range(size)])


def stage_kernel(codes_ref, *refs, first, last, scale, picks):
    q_ref, k_own, k_other, v_own, v_other = refs[:5]
    rest = list(refs[5:])
    state_in = None if first else [rest.pop(0) for _ in range(3)]
    if last:
        o_ref = rest.pop(0)
    else:
        m_ref, l_ref, acc_ref = [rest.pop(0) for _ in range(3)]
    keys, values, sems = rest[:3]
    if last:
        m_ref, l_ref, acc_ref = rest[3:]
    blocks, width, rows = acc_ref.shape

    copies = []
    for n, (source, target, at) in enumerate(
        ((k_own, keys, 0), (v_own, values, 0), (k_other, keys, blocks), (v_other, values, blocks))
    ):
        copy = pltpu.make_async_copy(source, target.at[pl.ds(at, blocks)], sems.at[n])
        copy.start()
        copies.append(copy)
    if not first:
        for new, old in zip((m_ref, l_ref, acc_ref), state_in):
            new[...] = old[...]

    def task(q, k, diagonal):
        for c in range(rows // CHUNK):
            cols = slice(c * CHUNK, (c + 1) * CHUNK)
            scores = lax.dot_general(
                keys[k], q_ref[q, cols, :], (((1,), (1,)), ((), ())), preferred_element_type=jnp.float32
            )
            if diagonal:
                kpos = lax.broadcasted_iota(jnp.int32, scores.shape, 0)
                qpos = lax.broadcasted_iota(jnp.int32, scores.shape, 1) + c * CHUNK
                scores = jnp.where(kpos <= qpos, scores, -jnp.inf)
            top = jnp.max(scores, axis=0, keepdims=True)
            if not diagonal:
                old = m_ref[q, :, cols]
                top = jnp.maximum(top, old)
            weights = jnp.exp2((scores - top) * (scale * LOG2E))
            total = jnp.sum(weights, axis=0, keepdims=True)
            part = lax.dot_general(
                values[k], weights.astype(jnp.bfloat16), (((0,), (0,)), ((), ())),
                preferred_element_type=jnp.float32,
            )
            m_ref[q, :, cols] = top
            if diagonal:
                l_ref[q, :, cols] = total
                acc_ref[q, :, cols] = part
            else:
                factor = jnp.exp2((old - top) * (scale * LOG2E))
                l_ref[q, :, cols] = l_ref[q, :, cols] * factor + total
                acc_ref[q, :, cols] = acc_ref[q, :, cols] * factor + part

    copies[0].wait()
    copies[1].wait()
    if first:

        @pl.loop(0, blocks)
        def _(q):
            task(q, q, True)

    copies[2].wait()
    copies[3].wait()

    @pl.loop(0, blocks * picks)
    def _(t):
        code = codes_ref[t]

        @pl.when(code >= 0)
        def _():
            task(t // picks, code, False)

    if last:

        @pl.loop(0, blocks)
        def _(q):
            o_ref[q] = (acc_ref[q] / l_ref[q]).T.astype(o_ref.dtype)


def attend_stage(codes, queries, keys, values, state, last, picks, tasks):
    blocks, rows, width = keys[0].shape
    first = state is None
    vmem, hbm = pl.BlockSpec(memory_space=pltpu.VMEM), pl.BlockSpec(memory_space=pl.ANY)
    state_shapes = (
        jax.ShapeDtypeStruct((blocks, 1, rows), jnp.float32),
        jax.ShapeDtypeStruct((blocks, 1, rows), jnp.float32),
        jax.ShapeDtypeStruct((blocks, width, rows), jnp.float32),
    )
    out_shape = jax.ShapeDtypeStruct((blocks, rows, width), jnp.bfloat16) if last else state_shapes
    return pl.pallas_call(
        functools.partial(stage_kernel, first=first, last=last, scale=width**-0.5, picks=picks),
        out_shape=out_shape,
        in_specs=[pl.BlockSpec(memory_space=pltpu.SMEM), vmem] + [hbm] * 4 + [vmem] * (0 if first else 3),
        out_specs=vmem if last else (vmem,) * 3,
        scratch_shapes=[
            pltpu.VMEM((2 * blocks, rows, width), jnp.bfloat16),
            pltpu.VMEM((2 * blocks, rows, width), jnp.bfloat16),
            pltpu.SemaphoreType.DMA((4,)),
        ]
        + [pltpu.VMEM(s.shape, s.dtype) for s in (state_shapes if last else ())],
        cost_estimate=pl.CostEstimate(
            flops=tasks * 16 * rows * rows * width,
            bytes_accessed=8 * blocks * rows * width,
            transcendentals=tasks * rows * rows,
        ),
    )(codes, queries, keys[0], keys[1], values[0], values[1], *(state or ()))


def body(query_rows, key_rows, value_rows, block_picks, out_weight):
    ny, nz, nx = lax.axis_size("y"), lax.axis_size("z"), lax.axis_size("x")
    y, z, x, c = (lax.axis_index(a) for a in ("y", "z", "x", "c"))
    tok_rows, feature = query_rows.shape
    blocks, heads, picks = block_picks.shape
    rows, width = tok_rows // blocks, feature // heads
    out_cols = out_weight.shape[1]

    def swap(array):
        own = lax.dynamic_index_in_dim(array, c, 0, keepdims=False)
        other = shift(lax.dynamic_index_in_dim(array, 1 - c, 0, keepdims=False), "c", 1)
        return jnp.stack((own, other))

    def head_tile(pair, h):
        which = (h >> (heads.bit_length() - 1)) ^ c
        at = (which, jnp.int32(0), (h & (heads - 1)) * width)
        return lax.dynamic_slice(pair, at, (1, pair.shape[1], width))[0]

    pick_rows = jnp.pad(block_picks.astype(jnp.bfloat16), ((0, 0), (0, 0), (0, width - picks)))
    pick_rows = jnp.pad(pick_rows.reshape(blocks, 1, feature), ((0, 0), (0, PAD - 1), (0, 0)))
    key_pair = swap(key_rows.reshape(blocks, rows, feature))
    value_pair = swap(value_rows.reshape(blocks, rows, feature))
    query_pair = swap(jnp.concatenate((query_rows.reshape(blocks, rows, feature), pick_rows), 1))
    weight_other = shift(out_weight, "c", 1)

    def reach(by):
        return (z + by) & (nz - 1)

    steps = (3, -3, 2, -2, 1, -1)
    key_at, value_at, query_at = [None] * nz, [None] * nz, [None] * nz
    half = nz // 2
    key_at[half] = shift(shift(head_tile(key_pair, reach(half)), "z", 2), "z", 2)
    value_at[half] = shift(shift(head_tile(value_pair, reach(half)), "z", -2), "z", -2)
    for by in steps:
        pair = jnp.stack((head_tile(key_pair, reach(by)), head_tile(value_pair, reach(by))))
        pair = shift(pair, "z", by)
        key_at[by % nz], value_at[by % nz] = pair[0], pair[1]
    key_at[0], value_at[0] = head_tile(key_pair, z), head_tile(value_pair, z)
    query_at[half] = shift(shift(head_tile(query_pair, reach(half)), "z", 2), "z", 2)
    for by in steps:
        query_at[by % nz] = shift(head_tile(query_pair, reach(by)), "z", by)
    query_at[0] = head_tile(query_pair, z)

    keys0, values0, queries = jnp.stack(key_at), jnp.stack(value_at), jnp.stack(query_at)

    keys, values = {0: keys0}, {0: values0}
    keys[1], values[1] = shift(keys0, "y", 1), shift(values0, "y", 1)
    keys[3], values[3] = shift(keys0, "y", -1), shift(values0, "y", -1)
    keys[2], values[2] = shift(keys[1], "y", 1), shift(values[3], "y", -1)

    mine = queries[:, rows, :picks].astype(jnp.int32)
    codes = {n: [] for n in range(ny)}
    for s in range(picks):
        entry = mine[:, s]
        fresh = entry >= 0
        for t in range(s):
            fresh = fresh & (entry != mine[:, t])
        block = jnp.maximum(entry, 0)
        code = ((z - block // blocks) & (nz - 1)) + nz * ((block & (blocks - 1)) ^ c)
        below = y - block // (nz * blocks)
        for n in range(ny):
            codes[n].append(jnp.where(fresh & (below == n), code, -1))
    state = None
    for n, tasks in ((0, 16), (1, 8), (3, 8), (2, 8)):
        table = jnp.stack(codes[n], 1).reshape(-1)
        pair_k = (keys[n], shift(keys[n], "c", 1))
        pair_v = (values[n], shift(values[n], "c", 1))
        state = attend_stage(table, queries, pair_k, pair_v, state, n == 2, picks, tasks)
    out = state

    back = [None] * nz
    back[half] = shift(shift(out[half], "z", -2), "z", -2)
    for by in steps:
        back[by % nz] = shift(out[by % nz], "z", -by)
    back[0] = out[0]
    attended = jnp.concatenate(back, 1)

    planes = {0: attended}
    planes[1], planes[3] = shift(attended, "x", 1), shift(attended, "x", -1)
    cut = nz * width // 2
    planes[2] = jnp.concatenate((shift(planes[1][:, :cut], "x", 1), shift(planes[3][:, cut:], "x", -1)), 1)

    weights = jnp.concatenate((out_weight, weight_other), 1).reshape(nx, nz, width, 2 * out_cols)
    order = (z + jnp.arange(nz)) & (nz - 1)
    total = None
    for n in (0, 1, 3, 2):
        part = lax.dynamic_index_in_dim(weights, (x - n) & (nx - 1), 0, keepdims=False)
        part = jnp.take(part, order, axis=0).reshape(nz * width, 2 * out_cols)
        product = jnp.dot(planes[n], part, preferred_element_type=jnp.float32)
        total = product if total is None else total + product
    total = total.astype(jnp.bfloat16)
    near, far = total[:, :out_cols], shift(total[:, out_cols:], "c", 1)
    return jnp.where(c == 0, jnp.concatenate((near, far)), jnp.concatenate((far, near)))


def solution(mesh):
    finer = Mesh(mesh.devices.reshape(4, 8, 4, 2), ("y", "z", "x", "c"))
    seq, head = ("y", "z"), ("x", "c")
    return jax.shard_map(
        body,
        mesh=finer,
        in_specs=(
            P(seq, head),
            P(seq, head),
            P(seq, head),
            P(seq, head, None),
            P(None, head),
        ),
        out_specs=P(seq, head),
        check_vma=False,
    )
```

```python
import functools

import jax
import jax.numpy as jnp
from jax import lax
from jax.experimental import pallas as pl
from jax.experimental.pallas import tpu as pltpu
from jax.sharding import Mesh
from jax.sharding import PartitionSpec as P


LOG2E = 1.4426950408889634
CHUNK = 128
PAD = 16
ORDER = (4, 3, -3, 2, -2, 1, -1)


def shift(array, axis, by):
    size = lax.axis_size(axis)
    return lax.ppermute(array, axis, [(i, (i + by) % size) for i in range(size)])


def stage_kernel(codes_ref, q_ref, *refs, first, last, scale, picks, parts):
    sources, rest = refs[: 2 * parts], list(refs[2 * parts :])
    state_in = () if first else [rest.pop(0) for _ in range(3)]
    if last:
        o_ref, keys, values, sems, m_ref, l_ref, acc_ref = rest
    else:
        m_ref, l_ref, acc_ref, keys, values, sems = rest
    blocks, _, rows = acc_ref.shape

    copies = []
    for n in range(parts):
        for source, target in ((sources[2 * n], keys), (sources[2 * n + 1], values)):
            copy = pltpu.make_async_copy(source, target.at[pl.ds(n * blocks, blocks)], sems.at[len(copies)])
            copy.start()
            copies.append(copy)
    for new, old in zip((m_ref, l_ref, acc_ref), state_in):
        new[...] = old[...]

    def task(q, k, diagonal):
        @pl.loop(0, rows // CHUNK)
        def _(c):
            cols = pl.ds(pl.multiple_of(c * CHUNK, CHUNK), CHUNK)
            scores = lax.dot_general(
                keys[k], q_ref[q, cols, :], (((1,), (1,)), ((), ())), preferred_element_type=jnp.float32
            )
            if diagonal:
                kpos = lax.broadcasted_iota(jnp.int32, scores.shape, 0)
                qpos = lax.broadcasted_iota(jnp.int32, scores.shape, 1) + c * CHUNK
                scores = jnp.where(kpos <= qpos, scores, -jnp.inf)
            top = jnp.max(scores, axis=0, keepdims=True)
            if not diagonal:
                old = m_ref[q, :, cols]
                top = jnp.maximum(top, old)
            weights = jnp.exp2((scores - top) * (scale * LOG2E))
            total = jnp.sum(weights, axis=0, keepdims=True)
            part = lax.dot_general(
                values[k], weights.astype(jnp.bfloat16), (((0,), (0,)), ((), ())),
                preferred_element_type=jnp.float32,
            )
            m_ref[q, :, cols] = top
            if diagonal:
                l_ref[q, :, cols] = total
                acc_ref[q, :, cols] = part
            else:
                factor = jnp.exp2((old - top) * (scale * LOG2E))
                l_ref[q, :, cols] = l_ref[q, :, cols] * factor + total
                acc_ref[q, :, cols] = acc_ref[q, :, cols] * factor + part

    if first:
        copies[0].wait()
        copies[1].wait()

        @pl.loop(0, blocks)
        def _(q):
            task(q, q, True)

    for copy in copies[2 if first else 0 :]:
        copy.wait()

    @pl.loop(0, blocks * picks)
    def _(t):
        code = codes_ref[t]

        @pl.when(code >= 0)
        def _():
            task(t // picks, code, False)

    if last:

        @pl.loop(0, blocks)
        def _(q):
            o_ref[q] = (acc_ref[q] / l_ref[q]).T.astype(o_ref.dtype)


def attend_stage(codes, queries, sources, state, last, picks, tasks):
    blocks, rows, width = sources[0][0].shape
    first = state is None
    parts = len(sources)
    vmem, hbm = pl.BlockSpec(memory_space=pltpu.VMEM), pl.BlockSpec(memory_space=pl.ANY)
    state_shapes = (
        jax.ShapeDtypeStruct((blocks, 1, rows), jnp.float32),
        jax.ShapeDtypeStruct((blocks, 1, rows), jnp.float32),
        jax.ShapeDtypeStruct((blocks, width, rows), jnp.float32),
    )
    out_shape = jax.ShapeDtypeStruct((blocks, rows, width), jnp.bfloat16) if last else state_shapes
    return pl.pallas_call(
        functools.partial(stage_kernel, first=first, last=last, scale=width**-0.5, picks=picks, parts=parts),
        out_shape=out_shape,
        in_specs=[pl.BlockSpec(memory_space=pltpu.SMEM), vmem] + [hbm] * (2 * parts) + [vmem] * (0 if first else 3),
        out_specs=vmem if last else (vmem,) * 3,
        scratch_shapes=[
            pltpu.VMEM((parts * blocks, rows, width), jnp.bfloat16),
            pltpu.VMEM((parts * blocks, rows, width), jnp.bfloat16),
            pltpu.SemaphoreType.DMA((2 * parts,)),
        ]
        + [pltpu.VMEM(s.shape, s.dtype) for s in (state_shapes if last else ())],
        cost_estimate=pl.CostEstimate(
            flops=tasks * 16 * rows * rows * width,
            bytes_accessed=4 * parts * blocks * rows * width,
            transcendentals=tasks * rows * rows,
        ),
    )(codes, queries, *(r for pair in sources for r in pair), *(state or ()))


def program(query_rows, key_rows, value_rows, block_picks, out_weight):
    nz, nx = lax.axis_size("z"), lax.axis_size("x")
    y, z, x, c = (lax.axis_index(a) for a in ("y", "z", "x", "c"))
    tok_rows, feature = query_rows.shape
    blocks, heads, picks = block_picks.shape
    rows, width = tok_rows // blocks, feature // heads
    out_cols = out_weight.shape[1]

    def swap(array):
        own = lax.dynamic_index_in_dim(array, c, 0, keepdims=False)
        other = shift(lax.dynamic_index_in_dim(array, 1 - c, 0, keepdims=False), "c", 1)
        return jnp.stack((own, other))

    def spread(pair):
        got = []
        for s in range(nz):
            h = (z + s) & (nz - 1)
            which = (h >> (heads.bit_length() - 1)) ^ c
            at = (which, jnp.int32(0), (h & (heads - 1)) * width)
            got.append(lax.dynamic_slice(pair, at, (1, pair.shape[1], width))[0])
        for by in ORDER:
            got[by % nz] = shift(got[by % nz], "z", by)
        return jnp.stack(got)

    key_pair = swap(key_rows.reshape(blocks, rows, feature))
    value_pair = swap(value_rows.reshape(blocks, rows, feature))
    pick_rows = jnp.pad(block_picks.astype(jnp.bfloat16), ((0, 0), (0, 0), (0, width - picks)))
    pick_rows = jnp.pad(pick_rows.reshape(blocks, 1, feature), ((0, 0), (0, PAD - 1), (0, 0)))
    query_pair = swap(jnp.concatenate((query_rows.reshape(blocks, rows, feature), pick_rows), 1))
    weight_other = shift(out_weight, "c", 1)

    keys, values = {}, {}
    keys[0] = spread(key_pair)
    keys[1], keys[3] = shift(keys[0], "y", 1), shift(keys[0], "y", -1)
    values[0] = spread(value_pair)
    values[1], values[3] = shift(values[0], "y", 1), shift(values[0], "y", -1)
    keys[2], values[2] = shift(keys[1], "y", 1), shift(values[3], "y", -1)
    queries = spread(query_pair)

    def plane_weight(n):
        at = (((x - n) & (nx - 1)) * nz * width, jnp.int32(0))
        size = (nz * width, out_cols)
        return jnp.concatenate([lax.dynamic_slice(w, at, size) for w in (out_weight, weight_other)], 1)

    early = jnp.concatenate([plane_weight(n) for n in (0, 1, 3)])
    late = plane_weight(2)

    mine = queries[:, rows, :picks].astype(jnp.int32)
    fresh = mine >= 0
    for gap in range(1, picks):
        same = mine[:, gap:] == mine[:, :-gap]
        fresh = fresh & ~jnp.pad(same, ((0, 0), (gap, 0)))
    block = jnp.maximum(mine, 0)
    code = ((z - block // blocks) & (nz - 1)) + nz * ((block & (blocks - 1)) ^ c)
    below = jnp.where(fresh, y - block // (nz * blocks), -1)
    code_of = {n: jnp.where(below == n, code, -1).reshape(-1) for n in (0, 2)}
    code_of[1] = jnp.where(below == 1, code, jnp.where(below == 3, code + 2 * nz, -1)).reshape(-1)

    def sources(n):
        return [(keys[n], values[n]), (shift(keys[n], "c", 1), shift(values[n], "c", 1))]

    queries, early, late = lax.optimization_barrier((queries, early, late))
    state = attend_stage(code_of[0], queries, sources(0), None, False, picks, 16)
    state = attend_stage(code_of[1], queries, sources(1) + sources(3), state, False, picks, 16)
    out = attend_stage(code_of[2], queries, sources(2), state, True, picks, 8)

    attended = jnp.zeros((rows, nz * width), jnp.bfloat16)
    back = {0: out[0]}
    for by in ORDER:
        back[by % nz] = shift(out[by % nz], "z", -by)
    for s in (0, 1, 7, 2, 6, 3, 5, 4):
        attended = lax.dynamic_update_slice(attended, back[s], (jnp.int32(0), ((z + s) & (nz - 1)) * width))

    up, down = shift(attended, "x", 1), shift(attended, "x", -1)
    cut = nz * width // 2
    far = (shift(up[:, :cut], "x", 1), shift(down[:, cut:], "x", -1))
    total = jnp.dot(jnp.concatenate((attended, up, down), 1), early, preferred_element_type=jnp.float32)
    total = lax.optimization_barrier(total)
    total = total + jnp.dot(jnp.concatenate(far, 1), late, preferred_element_type=jnp.float32)
    total = total.astype(jnp.bfloat16)
    near, other = total[:, :out_cols], shift(total[:, out_cols:], "c", 1)
    return jnp.where(c == 0, jnp.concatenate((near, other)), jnp.concatenate((other, near)))


def solution(mesh):
    finer = Mesh(mesh.devices.reshape(4, 8, 4, 2), ("y", "z", "x", "c"))
    seq, head = ("y", "z"), ("x", "c")
    return jax.shard_map(
        program,
        mesh=finer,
        in_specs=(
            P(seq, head),
            P(seq, head),
            P(seq, head),
            P(seq, head, None),
            P(None, head),
        ),
        out_specs=P(seq, head),
        check_vma=False,
    )
```

```python
import functools

import jax
import jax.numpy as jnp
from jax import lax
from jax.experimental import pallas as pl
from jax.experimental.pallas import tpu as pltpu
from jax.sharding import Mesh
from jax.sharding import PartitionSpec as P


LOG2E = 1.4426950408889634
CHUNK = 512
PAD = 16
ORDER = (4, 3, -3, 2, -2, 1, -1)


def shift(array, axis, by):
    size = lax.axis_size(axis)
    return lax.ppermute(array, axis, [(i, (i + by) % size) for i in range(size)])


def stage_kernel(codes_ref, q_ref, *refs, first, last, scale, picks, parts):
    sources, rest = refs[: 2 * parts], list(refs[2 * parts :])
    state_in = () if first else [rest.pop(0) for _ in range(3)]
    if last:
        *outs, keys, values, sems, m_ref, l_ref, acc_ref = rest
    else:
        m_ref, l_ref, acc_ref, keys, values, sems = rest
    blocks, _, rows = acc_ref.shape

    copies = []
    for n in range(parts):
        for source, target in ((sources[2 * n], keys), (sources[2 * n + 1], values)):
            copy = pltpu.make_async_copy(source, target.at[pl.ds(n * blocks, blocks)], sems.at[len(copies)])
            copy.start()
            copies.append(copy)
    for new, old in zip((m_ref, l_ref, acc_ref), state_in):
        new[...] = old[...]

    def task(q, k, diagonal):
        for c in range(rows // CHUNK):
            cols = slice(c * CHUNK, (c + 1) * CHUNK)
            scores = lax.dot_general(
                keys[k], q_ref[q, cols, :], (((1,), (1,)), ((), ())), preferred_element_type=jnp.float32
            )
            if diagonal:
                kpos = lax.broadcasted_iota(jnp.int32, scores.shape, 0)
                qpos = lax.broadcasted_iota(jnp.int32, scores.shape, 1) + c * CHUNK
                scores = jnp.where(kpos <= qpos, scores, -jnp.inf)
            top = jnp.max(scores, axis=0, keepdims=True)
            if not diagonal:
                old = m_ref[q, :, cols]
                top = jnp.maximum(top, old)
            weights = jnp.exp2((scores - top) * (scale * LOG2E))
            total = jnp.sum(weights, axis=0, keepdims=True)
            part = lax.dot_general(
                values[k], weights.astype(jnp.bfloat16), (((0,), (0,)), ((), ())),
                preferred_element_type=jnp.float32,
            )
            m_ref[q, :, cols] = top
            if diagonal:
                l_ref[q, :, cols] = total
                acc_ref[q, :, cols] = part
            else:
                factor = jnp.exp2((old - top) * (scale * LOG2E))
                l_ref[q, :, cols] = l_ref[q, :, cols] * factor + total
                acc_ref[q, :, cols] = acc_ref[q, :, cols] * factor + part

    if first:
        copies[0].wait()
        copies[1].wait()

        @pl.loop(0, blocks)
        def _(q):
            task(q, q, True)

    for copy in copies[2 if first else 0 :]:
        copy.wait()

    @pl.loop(0, blocks * picks)
    def _(t):
        code = codes_ref[t]

        @pl.when(code >= 0)
        def _():
            task(t // picks, code, False)

    if last:

        for q, o_ref in enumerate(outs):
            o_ref[...] = (acc_ref[q] / l_ref[q]).T.astype(o_ref.dtype)


def attend_stage(codes, queries, sources, state, last, picks, tasks):
    blocks, rows, width = sources[0][0].shape
    first = state is None
    parts = len(sources)
    vmem, hbm = pl.BlockSpec(memory_space=pltpu.VMEM), pl.BlockSpec(memory_space=pl.ANY)
    state_shapes = (
        jax.ShapeDtypeStruct((blocks, 1, rows), jnp.float32),
        jax.ShapeDtypeStruct((blocks, 1, rows), jnp.float32),
        jax.ShapeDtypeStruct((blocks, width, rows), jnp.float32),
    )
    out_shape = (jax.ShapeDtypeStruct((rows, width), jnp.bfloat16),) * blocks if last else state_shapes
    return pl.pallas_call(
        functools.partial(stage_kernel, first=first, last=last, scale=width**-0.5, picks=picks, parts=parts),
        out_shape=out_shape,
        in_specs=[pl.BlockSpec(memory_space=pltpu.SMEM), vmem] + [hbm] * (2 * parts) + [vmem] * (0 if first else 3),
        out_specs=(vmem,) * len(out_shape),
        scratch_shapes=[
            pltpu.VMEM((parts * blocks, rows, width), jnp.bfloat16),
            pltpu.VMEM((parts * blocks, rows, width), jnp.bfloat16),
            pltpu.SemaphoreType.DMA((2 * parts,)),
        ]
        + [pltpu.VMEM(s.shape, s.dtype) for s in (state_shapes if last else ())],
        cost_estimate=pl.CostEstimate(
            flops=tasks * 16 * rows * rows * width,
            bytes_accessed=4 * parts * blocks * rows * width,
            transcendentals=tasks * rows * rows,
        ),
    )(codes, queries, *(r for pair in sources for r in pair), *(state or ()))


def program(query_rows, key_rows, value_rows, block_picks, out_weight):
    nz, nx = lax.axis_size("z"), lax.axis_size("x")
    y, z, x, c = (lax.axis_index(a) for a in ("y", "z", "x", "c"))
    tok_rows, feature = query_rows.shape
    blocks, heads, picks = block_picks.shape
    rows, width = tok_rows // blocks, feature // heads
    out_cols = out_weight.shape[1]

    def swap(array):
        own = lax.dynamic_index_in_dim(array, c, 0, keepdims=False)
        other = shift(lax.dynamic_index_in_dim(array, 1 - c, 0, keepdims=False), "c", 1)
        return jnp.stack((own, other))

    def spread(pair):
        got = []
        for s in range(nz):
            h = (z + s) & (nz - 1)
            which = (h >> (heads.bit_length() - 1)) ^ c
            at = (which, jnp.int32(0), (h & (heads - 1)) * width)
            got.append(lax.dynamic_slice(pair, at, (1, pair.shape[1], width))[0])
        for by in ORDER:
            got[by % nz] = shift(got[by % nz], "z", by)
        return jnp.stack(got)

    key_pair = swap(key_rows.reshape(blocks, rows, feature))
    value_pair = swap(value_rows.reshape(blocks, rows, feature))
    pick_rows = jnp.pad(block_picks.astype(jnp.bfloat16), ((0, 0), (0, 0), (0, width - picks)))
    pick_rows = jnp.pad(pick_rows.reshape(blocks, 1, feature), ((0, 0), (0, PAD - 1), (0, 0)))
    query_pair = swap(jnp.concatenate((query_rows.reshape(blocks, rows, feature), pick_rows), 1))
    weight_other = shift(out_weight, "c", 1)

    keys, values = {}, {}
    keys[0] = spread(key_pair)
    keys[1], keys[3] = shift(keys[0], "y", 1), shift(keys[0], "y", -1)
    values[0] = spread(value_pair)
    values[1], values[3] = shift(values[0], "y", 1), shift(values[0], "y", -1)
    keys[2], values[2] = shift(keys[1], "y", 1), shift(values[3], "y", -1)
    queries = spread(query_pair)

    def plane_weight(n):
        at = (((x - n) & (nx - 1)) * nz * width, jnp.int32(0))
        size = (nz * width, out_cols)
        return jnp.concatenate([lax.dynamic_slice(w, at, size) for w in (out_weight, weight_other)], 1)

    plane_weights = tuple(plane_weight(n) for n in range(nx))

    mine = queries[:, rows, :picks].astype(jnp.int32)
    fresh = mine >= 0
    for gap in range(1, picks):
        same = mine[:, gap:] == mine[:, :-gap]
        fresh = fresh & ~jnp.pad(same, ((0, 0), (gap, 0)))
    block = jnp.maximum(mine, 0)
    code = ((z - block // blocks) & (nz - 1)) + nz * ((block & (blocks - 1)) ^ c)
    below = jnp.where(fresh, y - block // (nz * blocks), -1)
    near_code = jnp.where(below == 0, code, jnp.where(below == 1, code + 2 * nz, -1))
    near_code = jnp.where(below == 3, code + 4 * nz, near_code).reshape(-1)
    far_code = jnp.where(below == 2, code, -1).reshape(-1)

    def sources(n):
        return [(keys[n], values[n]), (shift(keys[n], "c", 1), shift(values[n], "c", 1))]

    queries, plane_weights = lax.optimization_barrier((queries, plane_weights))
    state = attend_stage(near_code, queries, sources(0) + sources(1) + sources(3), None, False, picks, 32)
    out = attend_stage(far_code, queries, sources(2), state, True, picks, 8)

    attended = jnp.zeros((rows, nz * width), jnp.bfloat16)
    back = {0: out[0]}
    for by in ORDER:
        back[by % nz] = shift(out[by % nz], "z", -by)
    for s in (0, 1, 7, 2, 6, 3, 5, 4):
        attended = lax.dynamic_update_slice(attended, back[s], (jnp.int32(0), ((z + s) & (nz - 1)) * width))

    up, down = shift(attended, "x", 1), shift(attended, "x", -1)
    cut = nz * width // 2
    far = (shift(up[:, :cut], "x", 1), shift(down[:, cut:], "x", -1))
    total = jnp.dot(attended, plane_weights[0], preferred_element_type=jnp.float32)
    total = total + jnp.dot(up, plane_weights[1], preferred_element_type=jnp.float32)
    total = total + jnp.dot(down, plane_weights[3], preferred_element_type=jnp.float32)
    total = lax.optimization_barrier(total)
    total = total + jnp.dot(jnp.concatenate(far, 1), plane_weights[2], preferred_element_type=jnp.float32)
    total = total.astype(jnp.bfloat16)
    near, other = total[:, :out_cols], shift(total[:, out_cols:], "c", 1)
    mixed = lax.dynamic_update_slice(jnp.zeros((tok_rows, out_cols), near.dtype), near, (c * rows, jnp.int32(0)))
    return lax.dynamic_update_slice(mixed, other, ((1 - c) * rows, jnp.int32(0)))


def solution(mesh):
    finer = Mesh(mesh.devices.reshape(4, 8, 4, 2), ("y", "z", "x", "c"))
    seq, head = ("y", "z"), ("x", "c")
    return jax.shard_map(
        program,
        mesh=finer,
        in_specs=(
            P(seq, head),
            P(seq, head),
            P(seq, head),
            P(seq, head, None),
            P(None, head),
        ),
        out_specs=P(seq, head),
        check_vma=False,
    )
```

```python
import functools

import jax
import jax.numpy as jnp
from jax import lax
from jax.experimental import pallas as pl
from jax.experimental.pallas import tpu as pltpu
from jax.sharding import Mesh
from jax.sharding import PartitionSpec as P


LOG2E = 1.4426950408889634
CHUNK = 512
PAD = 16
TILE = 256
ORDER = (4, 3, -3, 2, -2, 1, -1)


def shift(array, axis, by):
    size = lax.axis_size(axis)
    return lax.ppermute(array, axis, [(i, (i + by) % size) for i in range(size)])


def stage_kernel(codes_ref, q_ref, *refs, first, last, scale, picks, parts):
    sources, rest = refs[: 2 * parts], list(refs[2 * parts :])
    state_in = () if first else [rest.pop(0) for _ in range(3)]
    if last:
        *outs, keys, values, sems, m_ref, l_ref, acc_ref = rest
    else:
        m_ref, l_ref, acc_ref, keys, values, sems = rest
    blocks, _, rows = acc_ref.shape

    copies = []
    for n in range(parts):
        for source, target in ((sources[2 * n], keys), (sources[2 * n + 1], values)):
            copy = pltpu.make_async_copy(source, target.at[pl.ds(n * blocks, blocks)], sems.at[len(copies)])
            copy.start()
            copies.append(copy)
    for new, old in zip((m_ref, l_ref, acc_ref), state_in):
        new[...] = old[...]

    def task(q, k, diagonal):
        for c in range(rows // CHUNK):
            cols = slice(c * CHUNK, (c + 1) * CHUNK)
            scores = lax.dot_general(
                keys[k], q_ref[q, cols, :], (((1,), (1,)), ((), ())), preferred_element_type=jnp.float32
            )
            if diagonal:
                kpos = lax.broadcasted_iota(jnp.int32, scores.shape, 0)
                qpos = lax.broadcasted_iota(jnp.int32, scores.shape, 1) + c * CHUNK
                scores = jnp.where(kpos <= qpos, scores, -jnp.inf)
            top = jnp.max(scores, axis=0, keepdims=True)
            if not diagonal:
                old = m_ref[q, :, cols]
                top = jnp.maximum(top, old)
            weights = jnp.exp2((scores - top) * (scale * LOG2E))
            total = jnp.sum(weights, axis=0, keepdims=True)
            part = lax.dot_general(
                values[k], weights.astype(jnp.bfloat16), (((0,), (0,)), ((), ())),
                preferred_element_type=jnp.float32,
            )
            m_ref[q, :, cols] = top
            if diagonal:
                l_ref[q, :, cols] = total
                acc_ref[q, :, cols] = part
            else:
                factor = jnp.exp2((old - top) * (scale * LOG2E))
                l_ref[q, :, cols] = l_ref[q, :, cols] * factor + total
                acc_ref[q, :, cols] = acc_ref[q, :, cols] * factor + part

    if first:
        copies[0].wait()
        copies[1].wait()

        @pl.loop(0, blocks)
        def _(q):
            task(q, q, True)

    for copy in copies[2 if first else 0 :]:
        copy.wait()

    @pl.loop(0, blocks * picks)
    def _(t):
        code = codes_ref[t]

        @pl.when(code >= 0)
        def _():
            task(t // picks, code, False)

    if last:

        z = codes_ref[blocks * picks]

        @pl.loop(0, blocks)
        def _(q):
            outs[0][(z - q) & (blocks - 1)] = (acc_ref[q] / l_ref[q]).T.astype(outs[0].dtype)


def attend_stage(codes, queries, sources, state, last, picks, tasks):
    blocks, rows, width = sources[0][0].shape
    first = state is None
    parts = len(sources)
    vmem, hbm = pl.BlockSpec(memory_space=pltpu.VMEM), pl.BlockSpec(memory_space=pl.ANY)
    state_shapes = (
        jax.ShapeDtypeStruct((blocks, 1, rows), jnp.float32),
        jax.ShapeDtypeStruct((blocks, 1, rows), jnp.float32),
        jax.ShapeDtypeStruct((blocks, width, rows), jnp.float32),
    )
    out_shape = (jax.ShapeDtypeStruct((blocks, rows, width), jnp.bfloat16),) if last else state_shapes
    return pl.pallas_call(
        functools.partial(stage_kernel, first=first, last=last, scale=width**-0.5, picks=picks, parts=parts),
        out_shape=out_shape,
        in_specs=[pl.BlockSpec(memory_space=pltpu.SMEM), vmem] + [hbm] * (2 * parts) + [vmem] * (0 if first else 3),
        out_specs=(vmem,) * len(out_shape),
        scratch_shapes=[
            pltpu.VMEM((parts * blocks, rows, width), jnp.bfloat16),
            pltpu.VMEM((parts * blocks, rows, width), jnp.bfloat16),
            pltpu.SemaphoreType.DMA((2 * parts,)),
        ]
        + [pltpu.VMEM(s.shape, s.dtype) for s in (state_shapes if last else ())],
        cost_estimate=pl.CostEstimate(
            flops=tasks * 16 * rows * rows * width,
            bytes_accessed=4 * parts * blocks * rows * width,
            transcendentals=tasks * rows * rows,
        ),
    )(codes, queries, *(r for pair in sources for r in pair), *(state or ()))


def pack_kernel(at_ref, raw_ref, got_ref, *refs, heads):
    outs, (pair, sems) = refs[:-2], refs[-2:]
    z, c = at_ref[0], at_ref[1]
    copies = [
        pltpu.make_async_copy(raw_ref.at[c], pair.at[0], sems.at[0]),
        pltpu.make_async_copy(got_ref, pair.at[1], sems.at[1]),
    ]
    for copy in copies:
        copy.start()
    for copy in copies:
        copy.wait()
    rows, width = outs[0].shape
    step = rows // (4 if rows % 64 == 0 else 3)

    @pl.loop(0, rows // step)
    def _(r):
        lines = pl.ds(pl.multiple_of(r * step, 16), step)
        for s, out in enumerate(outs):
            h = (z + s) & (len(outs) - 1)
            which = (h >> (heads.bit_length() - 1)) ^ c
            cols = pl.ds(pl.multiple_of((h & (heads - 1)) * width, width), width)
            out[lines, :] = pair[which, lines, cols]


def pack(at, raw, got, heads, count):
    rows, feature = got.shape
    vmem, hbm = pl.BlockSpec(memory_space=pltpu.VMEM), pl.BlockSpec(memory_space=pl.ANY)
    return pl.pallas_call(
        functools.partial(pack_kernel, heads=heads),
        out_shape=(jax.ShapeDtypeStruct((rows, feature // heads), raw.dtype),) * count,
        in_specs=[pl.BlockSpec(memory_space=pltpu.SMEM), hbm, hbm],
        out_specs=(vmem,) * count,
        scratch_shapes=[pltpu.VMEM((2, rows, feature), raw.dtype), pltpu.SemaphoreType.DMA((2,))],
        cost_estimate=pl.CostEstimate(flops=1 << 20, bytes_accessed=8 * rows * feature, transcendentals=0),
    )(at, raw, got)


def project_kernel(x_ref, *refs, plan, planes, last):
    parts, refs = len(plan), list(refs)
    sources = [refs.pop(0) for _ in range(parts)]
    weights = [refs.pop(0) for _ in range(2)]
    acc_in = refs.pop(0) if last else None
    outs, (data, held, sems) = refs[:-3], refs[-3:]
    depth, cols = held.shape[2:]
    copies = []

    def start(source, target):
        copy = pltpu.make_async_copy(source, target, sems.at[len(copies)])
        copy.start()
        copies.append(copy)

    plane_rows = weights[0].shape[0] // planes
    for p, (n, offset) in enumerate(plan):
        start(sources[p], data.at[p])
        base = ((x_ref[0] - n) & (planes - 1)) * plane_rows + offset
        for h in range(2):
            start(weights[h].at[pl.ds(pl.multiple_of(base, depth), depth)], held.at[p, h])
    for copy in copies:
        copy.wait()

    def product(p, h, at):
        return jnp.dot(data[p], held[p, h, :, at], preferred_element_type=jnp.float32)

    @pl.loop(0, cols // TILE)
    def _(t):
        at = pl.ds(pl.multiple_of(t * TILE, TILE), TILE)
        if last:
            for h in range(2):
                total = acc_in[h, :, at]
                for p in range(parts):
                    total = total + product(p, h, at)
                outs[h][:, at] = total.astype(outs[h].dtype)
        else:

            @pl.loop(0, 2)
            def _(h):
                outs[0][h, :, at] = jnp.zeros(outs[0].shape[1:2] + (TILE,), jnp.float32)

                @pl.loop(0, parts)
                def _(p):
                    outs[0][h, :, at] += product(p, h, at)


def project(x, sources, plan, weights, planes, acc):
    rows, depth = sources[0].shape
    parts, cols, last = len(plan), weights[0].shape[1], acc is not None
    vmem, hbm = pl.BlockSpec(memory_space=pltpu.VMEM), pl.BlockSpec(memory_space=pl.ANY)
    if last:
        out_shape = (jax.ShapeDtypeStruct((rows, cols), jnp.bfloat16),) * 2
    else:
        out_shape = (jax.ShapeDtypeStruct((2, rows, cols), jnp.float32),)
    return pl.pallas_call(
        functools.partial(project_kernel, plan=plan, planes=planes, last=last),
        out_shape=out_shape,
        in_specs=[pl.BlockSpec(memory_space=pltpu.SMEM)] + [hbm] * (parts + 2) + [vmem] * last,
        out_specs=(vmem,) * len(out_shape),
        scratch_shapes=[
            pltpu.VMEM((parts, rows, depth), jnp.bfloat16),
            pltpu.VMEM((parts, 2, depth, cols), jnp.bfloat16),
            pltpu.SemaphoreType.DMA((3 * parts,)),
        ],
        cost_estimate=pl.CostEstimate(
            flops=4 * parts * rows * depth * cols,
            bytes_accessed=2 * parts * depth * (rows + 2 * cols),
            transcendentals=0,
        ),
    )(x.reshape(1), *sources, *weights, *((acc,) if last else ()))


def program(query_rows, key_rows, value_rows, block_picks, out_weight):
    nz, nx = lax.axis_size("z"), lax.axis_size("x")
    y, z, x, c = (lax.axis_index(a) for a in ("y", "z", "x", "c"))
    tok_rows, feature = query_rows.shape
    blocks, heads, picks = block_picks.shape
    rows, width = tok_rows // blocks, feature // heads
    out_cols = out_weight.shape[1]

    place = jnp.stack((z, c))

    def swap(array):
        return array, shift(lax.dynamic_index_in_dim(array, 1 - c, 0, keepdims=False), "c", 1)

    def spread(pair):
        got = list(pack(place, *pair, heads, nz))
        for by in ORDER:
            got[by % nz] = shift(got[by % nz], "z", by)
        return jnp.stack(got)

    key_pair = swap(key_rows.reshape(blocks, rows, feature))
    value_pair = swap(value_rows.reshape(blocks, rows, feature))
    pick_rows = jnp.pad(block_picks.astype(jnp.bfloat16), ((0, 0), (0, 0), (0, width - picks)))
    pick_rows = jnp.pad(pick_rows.reshape(blocks, 1, feature), ((0, 0), (0, PAD - 1), (0, 0)))
    query_pair = swap(jnp.concatenate((query_rows.reshape(blocks, rows, feature), pick_rows), 1))
    weight_other = shift(out_weight, "c", 1)

    keys, values = {}, {}
    keys[0] = spread(key_pair)
    keys[1], keys[3] = shift(keys[0], "y", 1), shift(keys[0], "y", -1)
    values[0] = spread(value_pair)
    values[1], values[3] = shift(values[0], "y", 1), shift(values[0], "y", -1)
    keys[2], values[2] = shift(keys[1], "y", 1), shift(values[3], "y", -1)
    queries = spread(query_pair)

    mine = queries[:, rows, :picks].astype(jnp.int32)
    fresh = mine >= 0
    for gap in range(1, picks):
        same = mine[:, gap:] == mine[:, :-gap]
        fresh = fresh & ~jnp.pad(same, ((0, 0), (gap, 0)))
    block = jnp.maximum(mine, 0)
    code = ((z - block // blocks) & (nz - 1)) + nz * ((block & (blocks - 1)) ^ c)
    below = jnp.where(fresh, y - block // (nz * blocks), -1)
    near_code = jnp.where(below == 0, code, jnp.where(below == 1, code + 2 * nz, -1))
    near_code = jnp.where(below == 3, code + 4 * nz, near_code).reshape(-1)
    far_code = jnp.where(below == 2, code, -1).reshape(-1)

    def sources(n):
        return [(keys[n], values[n]), (shift(keys[n], "c", 1), shift(values[n], "c", 1))]

    state = attend_stage(near_code, queries, sources(0) + sources(1) + sources(3), None, False, picks, 32)
    (out,) = attend_stage(jnp.append(far_code, z), queries, sources(2), state, True, picks, 8)

    attended = lax.all_to_all(out, "z", split_axis=0, concat_axis=0, tiled=True)
    attended = jnp.transpose(attended, (1, 0, 2)).reshape(rows, nz * width)

    up, down = shift(attended, "x", 1), shift(attended, "x", -1)
    cut = nz * width // 2
    far = (shift(up[:, :cut], "x", 1), shift(down[:, cut:], "x", -1))
    weights = (out_weight, weight_other)
    (total,) = project(x, (attended, up, down), ((0, 0), (1, 0), (3, 0)), weights, nx, None)
    near, other = project(x, far, ((2, 0), (2, cut)), weights, nx, total)
    other = shift(other, "c", 1)
    mixed = lax.dynamic_update_slice(jnp.zeros((tok_rows, out_cols), near.dtype), near, (c * rows, jnp.int32(0)))
    return lax.dynamic_update_slice(mixed, other, ((1 - c) * rows, jnp.int32(0)))


def solution(mesh):
    finer = Mesh(mesh.devices.reshape(4, 8, 4, 2), ("y", "z", "x", "c"))
    seq, head = ("y", "z"), ("x", "c")
    return jax.shard_map(
        program,
        mesh=finer,
        in_specs=(
            P(seq, head),
            P(seq, head),
            P(seq, head),
            P(seq, head, None),
            P(None, head),
        ),
        out_specs=P(seq, head),
        check_vma=False,
    )
```

```python
import functools

import jax
import jax.numpy as jnp
from jax import lax
from jax.experimental import pallas as pl
from jax.experimental.pallas import tpu as pltpu
from jax.sharding import Mesh
from jax.sharding import PartitionSpec as P


LOG2E = 1.4426950408889634
CHUNK = 512
PAD = 16
TILE = 256
ORDER = (4, 3, -3, 2, -2, 1, -1)


def shift(array, axis, by):
    size = lax.axis_size(axis)
    return lax.ppermute(array, axis, [(i, (i + by) % size) for i in range(size)])


def stage_kernel(codes_ref, q_ref, *refs, first, last, scale, picks, parts):
    sources, rest = refs[: 2 * parts], list(refs[2 * parts :])
    state_in = () if first else [rest.pop(0) for _ in range(3)]
    if last:
        *outs, keys, values, sems, m_ref, l_ref, acc_ref = rest
    else:
        m_ref, l_ref, acc_ref, keys, values, sems = rest
    blocks, _, rows = acc_ref.shape

    copies = []
    for n in range(parts):
        for source, target in ((sources[2 * n], keys), (sources[2 * n + 1], values)):
            copy = pltpu.make_async_copy(source, target.at[pl.ds(n * blocks, blocks)], sems.at[len(copies)])
            copy.start()
            copies.append(copy)
    for new, old in zip((m_ref, l_ref, acc_ref), state_in):
        new[...] = old[...]

    def task(q, k, diagonal):
        for c in range(rows // CHUNK):
            cols = slice(c * CHUNK, (c + 1) * CHUNK)
            scores = lax.dot_general(
                keys[k], q_ref[q, cols, :], (((1,), (1,)), ((), ())), preferred_element_type=jnp.float32
            )
            if diagonal:
                kpos = lax.broadcasted_iota(jnp.int32, scores.shape, 0)
                qpos = lax.broadcasted_iota(jnp.int32, scores.shape, 1) + c * CHUNK
                scores = jnp.where(kpos <= qpos, scores, -jnp.inf)
            top = jnp.max(scores, axis=0, keepdims=True)
            if not diagonal:
                old = m_ref[q, :, cols]
                top = jnp.maximum(top, old)
            weights = jnp.exp2((scores - top) * (scale * LOG2E))
            total = jnp.sum(weights, axis=0, keepdims=True)
            part = lax.dot_general(
                values[k], weights.astype(jnp.bfloat16), (((0,), (0,)), ((), ())),
                preferred_element_type=jnp.float32,
            )
            m_ref[q, :, cols] = top
            if diagonal:
                l_ref[q, :, cols] = total
                acc_ref[q, :, cols] = part
            else:
                factor = jnp.exp2((old - top) * (scale * LOG2E))
                l_ref[q, :, cols] = l_ref[q, :, cols] * factor + total
                acc_ref[q, :, cols] = acc_ref[q, :, cols] * factor + part

    if first:
        copies[0].wait()
        copies[1].wait()

        @pl.loop(0, blocks)
        def _(q):
            task(q, q, True)

    for copy in copies[2 if first else 0 :]:
        copy.wait()

    @pl.loop(0, blocks * picks)
    def _(t):
        code = codes_ref[t]

        @pl.when(code >= 0)
        def _():
            task(t // picks, code, False)

    if last:

        z = codes_ref[blocks * picks]

        @pl.loop(0, blocks)
        def _(q):
            outs[0][(z - q) & (blocks - 1)] = (acc_ref[q] / l_ref[q]).T.astype(outs[0].dtype)


def attend_stage(codes, queries, sources, state, last, picks, tasks):
    blocks, rows, width = sources[0][0].shape
    first = state is None
    parts = len(sources)
    vmem, hbm = pl.BlockSpec(memory_space=pltpu.VMEM), pl.BlockSpec(memory_space=pl.ANY)
    state_shapes = (
        jax.ShapeDtypeStruct((blocks, 1, rows), jnp.float32),
        jax.ShapeDtypeStruct((blocks, 1, rows), jnp.float32),
        jax.ShapeDtypeStruct((blocks, width, rows), jnp.float32),
    )
    out_shape = (jax.ShapeDtypeStruct((blocks, rows, width), jnp.bfloat16),) if last else state_shapes
    return pl.pallas_call(
        functools.partial(stage_kernel, first=first, last=last, scale=width**-0.5, picks=picks, parts=parts),
        out_shape=out_shape,
        in_specs=[pl.BlockSpec(memory_space=pltpu.SMEM), vmem] + [hbm] * (2 * parts) + [vmem] * (0 if first else 3),
        out_specs=(vmem,) * len(out_shape),
        scratch_shapes=[
            pltpu.VMEM((parts * blocks, rows, width), jnp.bfloat16),
            pltpu.VMEM((parts * blocks, rows, width), jnp.bfloat16),
            pltpu.SemaphoreType.DMA((2 * parts,)),
        ]
        + [pltpu.VMEM(s.shape, s.dtype) for s in (state_shapes if last else ())],
        cost_estimate=pl.CostEstimate(
            flops=tasks * 16 * rows * rows * width,
            bytes_accessed=4 * parts * blocks * rows * width,
            transcendentals=tasks * rows * rows,
        ),
    )(codes, queries, *(r for pair in sources for r in pair), *(state or ()))


def project_kernel(x_ref, *refs, plan, planes, last):
    parts, refs = len(plan), list(refs)
    sources = [refs.pop(0) for _ in range(parts)]
    weights = [refs.pop(0) for _ in range(2)]
    acc_in = refs.pop(0) if last else None
    outs, (data, held, sems) = refs[:-3], refs[-3:]
    depth, cols = held.shape[2:]
    copies = []

    def start(source, target):
        copy = pltpu.make_async_copy(source, target, sems.at[len(copies)])
        copy.start()
        copies.append(copy)

    plane_rows = weights[0].shape[0] // planes
    for p, (n, offset) in enumerate(plan):
        start(sources[p], data.at[p])
        base = ((x_ref[0] - n) & (planes - 1)) * plane_rows + offset
        for h in range(2):
            start(weights[h].at[pl.ds(pl.multiple_of(base, depth), depth)], held.at[p, h])
    for copy in copies:
        copy.wait()

    def product(p, h, at):
        return jnp.dot(data[p], held[p, h, :, at], preferred_element_type=jnp.float32)

    @pl.loop(0, cols // TILE)
    def _(t):
        at = pl.ds(pl.multiple_of(t * TILE, TILE), TILE)
        if last:
            for h in range(2):
                total = acc_in[h, :, at]
                for p in range(parts):
                    total = total + product(p, h, at)
                outs[h][:, at] = total.astype(outs[h].dtype)
        else:

            @pl.loop(0, 2)
            def _(h):
                outs[0][h, :, at] = jnp.zeros(outs[0].shape[1:2] + (TILE,), jnp.float32)

                @pl.loop(0, parts)
                def _(p):
                    outs[0][h, :, at] += product(p, h, at)


def project(x, sources, plan, weights, planes, acc):
    rows, depth = sources[0].shape
    parts, cols, last = len(plan), weights[0].shape[1], acc is not None
    vmem, hbm = pl.BlockSpec(memory_space=pltpu.VMEM), pl.BlockSpec(memory_space=pl.ANY)
    if last:
        out_shape = (jax.ShapeDtypeStruct((rows, cols), jnp.bfloat16),) * 2
    else:
        out_shape = (jax.ShapeDtypeStruct((2, rows, cols), jnp.float32),)
    return pl.pallas_call(
        functools.partial(project_kernel, plan=plan, planes=planes, last=last),
        out_shape=out_shape,
        in_specs=[pl.BlockSpec(memory_space=pltpu.SMEM)] + [hbm] * (parts + 2) + [vmem] * last,
        out_specs=(vmem,) * len(out_shape),
        scratch_shapes=[
            pltpu.VMEM((parts, rows, depth), jnp.bfloat16),
            pltpu.VMEM((parts, 2, depth, cols), jnp.bfloat16),
            pltpu.SemaphoreType.DMA((3 * parts,)),
        ],
        cost_estimate=pl.CostEstimate(
            flops=4 * parts * rows * depth * cols,
            bytes_accessed=2 * parts * depth * (rows + 2 * cols),
            transcendentals=0,
        ),
    )(x.reshape(1), *sources, *weights, *((acc,) if last else ()))


def program(query_rows, key_rows, value_rows, block_picks, out_weight):
    nz, nx = lax.axis_size("z"), lax.axis_size("x")
    y, z, x, c = (lax.axis_index(a) for a in ("y", "z", "x", "c"))
    tok_rows, feature = query_rows.shape
    blocks, heads, picks = block_picks.shape
    rows, width = tok_rows // blocks, feature // heads
    out_cols = out_weight.shape[1]

    def swap(array):
        own = lax.dynamic_index_in_dim(array, c, 0, keepdims=False)
        other = shift(lax.dynamic_index_in_dim(array, 1 - c, 0, keepdims=False), "c", 1)
        return jnp.stack((own, other))

    def spread(pair):
        got = []
        for s in range(nz):
            h = (z + s) & (nz - 1)
            which = (h >> (heads.bit_length() - 1)) ^ c
            at = (which, jnp.int32(0), (h & (heads - 1)) * width)
            got.append(lax.dynamic_slice(pair, at, (1, pair.shape[1], width))[0])
        for by in ORDER:
            got[by % nz] = shift(got[by % nz], "z", by)
        return jnp.stack(got)

    key_pair = swap(key_rows.reshape(blocks, rows, feature))
    value_pair = swap(value_rows.reshape(blocks, rows, feature))
    pick_rows = jnp.pad(block_picks.astype(jnp.bfloat16), ((0, 0), (0, 0), (0, width - picks)))
    pick_rows = jnp.pad(pick_rows.reshape(blocks, 1, feature), ((0, 0), (0, PAD - 1), (0, 0)))
    query_pair = swap(jnp.concatenate((query_rows.reshape(blocks, rows, feature), pick_rows), 1))
    weight_other = shift(out_weight, "c", 1)

    keys, values = {}, {}
    keys[0] = spread(key_pair)
    keys[1], keys[3] = shift(keys[0], "y", 1), shift(keys[0], "y", -1)
    values[0] = spread(value_pair)
    values[1], values[3] = shift(values[0], "y", 1), shift(values[0], "y", -1)
    keys[2], values[2] = shift(keys[1], "y", 1), shift(values[3], "y", -1)
    queries = spread(query_pair)

    mine = queries[:, rows, :picks].astype(jnp.int32)
    fresh = mine >= 0
    for gap in range(1, picks):
        same = mine[:, gap:] == mine[:, :-gap]
        fresh = fresh & ~jnp.pad(same, ((0, 0), (gap, 0)))
    block = jnp.maximum(mine, 0)
    code = ((z - block // blocks) & (nz - 1)) + nz * ((block & (blocks - 1)) ^ c)
    below = jnp.where(fresh, y - block // (nz * blocks), -1)
    near_code = jnp.where(below == 0, code, jnp.where(below == 1, code + 2 * nz, -1))
    near_code = jnp.where(below == 3, code + 4 * nz, near_code).reshape(-1)
    far_code = jnp.where(below == 2, code, -1).reshape(-1)

    def sources(n):
        return [(keys[n], values[n]), (shift(keys[n], "c", 1), shift(values[n], "c", 1))]

    state = attend_stage(near_code, queries, sources(0) + sources(1) + sources(3), None, False, picks, 32)
    (out,) = attend_stage(jnp.append(far_code, z), queries, sources(2), state, True, picks, 8)

    attended = lax.all_to_all(out, "z", split_axis=0, concat_axis=0, tiled=True)
    attended = jnp.transpose(attended, (1, 0, 2)).reshape(rows, nz * width)

    up, down = shift(attended, "x", 1), shift(attended, "x", -1)
    cut = nz * width // 2
    far = (shift(up[:, :cut], "x", 1), shift(down[:, cut:], "x", -1))
    weights = (out_weight, weight_other)
    (total,) = project(x, (attended, up, down), ((0, 0), (1, 0), (3, 0)), weights, nx, None)
    near, other = project(x, far, ((2, 0), (2, cut)), weights, nx, total)
    other = shift(other, "c", 1)
    mixed = lax.dynamic_update_slice(jnp.zeros((tok_rows, out_cols), near.dtype), near, (c * rows, jnp.int32(0)))
    return lax.dynamic_update_slice(mixed, other, ((1 - c) * rows, jnp.int32(0)))


def solution(mesh):
    finer = Mesh(mesh.devices.reshape(4, 8, 4, 2), ("y", "z", "x", "c"))
    seq, head = ("y", "z"), ("x", "c")
    return jax.shard_map(
        program,
        mesh=finer,
        in_specs=(
            P(seq, head),
            P(seq, head),
            P(seq, head),
            P(seq, head, None),
            P(None, head),
        ),
        out_specs=P(seq, head),
        check_vma=False,
    )
```
